128 devices in a mesh: cuts: 4 (over x_hi, core), dom: 16 (over y, z), vec: 2 (over x_lo).
Axes of the slice: x: 4 (x_hi: 2, x_lo: 2; x = x_hi * 2 + x_lo), y: 4, z: 4, core: 2. Of those that a mesh axis runs over, the one named last changes fastest.
Arguments:
- starts_old: bfloat16 [4, 2, 32, 1536, 768], P('cuts', None, 'vec', 'dom'), may hold values from -6 to 6
- y_operator: bfloat16 [768, 768], replicated, may hold values from -0.21875 to 0.21875
- coarse_inverse: bfloat16 [1536, 1536], P('vec'), may hold values from -1 to 2
- base_speed: float32 [1536, 768], P('dom'), may hold values from 0.5 to 1.5
- damping: float32 [32], P('vec'), may hold values from 0.5 to 3
- coupling: float32 [32], P('vec'), may hold values from 0.3 to 1.5
Outputs:
- ends_new: float32 [4, 2, 32, 1536, 768], P('cuts', None, 'vec', 'dom')
The draws below stay inside these ranges and needn't reach their ends.
All inputs are finite; a program needn't handle non-finite values.
Results may differ from the reference program's by a relative error of at most 0.0078.
Values may be sent and summed in bfloat16 or wider, within the bound.
A program may use at most 192 MiB of HBM per device.

```python
import math
import jax
import jax.numpy as jnp
import numpy as np
from jax import lax

WAVES = 32
NY = 768
NP = 16
NX = 1536
SLICES = 4


def draw_coarse_inverse(key, part):
    noise = jax.random.normal(key, (NX, NX), jnp.float32)
    matrix = jnp.eye(NX, dtype=jnp.float32) + 0.3 * noise / math.sqrt(NX)
    return matrix.astype(jnp.bfloat16)


def steps_of(stream_key, shape, shards, least, top_value):
    gain, own = 1.0, jax.random.fold_in(stream_key, 6)
    for axis_at, blocks in shards:
        steps = jnp.exp(jax.random.uniform(jax.random.fold_in(own, axis_at), (blocks,), jnp.float32, least / len(shards), top_value / len(shards)))
        gain = gain * jnp.repeat(steps, shape[axis_at] // blocks).reshape([-1 if axis == axis_at else 1 for axis in range(len(shape))])
    return gain


def bell_draw(own_key, extent, deviation, reach, pieces=(), held_as=jnp.bfloat16):
    gain = steps_of(own_key, extent, pieces, -0.22, 0.18) if pieces else 1.0
    drawn = jax.random.normal(own_key, extent, jnp.float32) * deviation * gain
    return jnp.minimum(jnp.maximum(drawn, -reach), reach).astype(held_as)


def setup_inputs(seed: int = 0) -> dict:
    keys = jax.random.split(jax.random.key(seed), 7)
    starts_old = bell_draw(keys[0], (SLICES, 2, WAVES, NX, NY), 1.0, 6.0, ((0, 4), (2, 2), (3, 16)))
    y_operator = bell_draw(keys[1], (NY, NY), NY ** -0.5, 0.21875)
    coarse_inverse = draw_coarse_inverse(jax.random.fold_in(keys[6], 71), 0)
    base_speed = jnp.clip(0.5 + 1.0 * jax.random.uniform(keys[3], (NX, NY), jnp.float32) ** steps_of(keys[3], (NX, NY), ((0, 16),), -0.2, 0.2), 0.5, 1.5)
    damping = jnp.clip(jnp.exp(math.log(3.0) - 1.7917595 * jax.random.uniform(keys[4], (WAVES,), jnp.float32) ** steps_of(keys[4], (WAVES,), ((0, 2),), -0.2, 0.2)), 0.5, 3.0)
    coupling = jnp.clip(jnp.exp(math.log(1.5) - 1.60943787 * jax.random.uniform(keys[5], (WAVES,), jnp.float32) ** steps_of(keys[5], (WAVES,), ((0, 2),), -0.2, 0.2)), 0.3, 1.5)
    return {"starts_old": starts_old, "y_operator": y_operator, "coarse_inverse": coarse_inverse, "base_speed": base_speed, "damping": damping, "coupling": coupling}


fine_step = 0.25
penalty = 2.0


def cheb_matrix(points_sub):
    indices = np.arange(points_sub)
    points = -np.cos(np.pi * indices / (points_sub - 1))
    edge_weight = np.where((indices == 0) | (indices == points_sub - 1), 2.0, 1.0)
    sign_table = np.where((indices[:, None] + indices[None, :]) % 2 == 0, 1.0, -1.0)
    identity_table = np.eye(points_sub)
    gap_matrix = points[:, None] - points[None, :] + identity_table
    off_diag = edge_weight[:, None] / edge_weight[None, :] * sign_table / gap_matrix * (1.0 - identity_table)
    return off_diag - off_diag.sum(axis=1)[:, None] * identity_table


def slope_of(values, y_operator, base_speed, damping, coupling, derivative):
    parts, wave_count, column_count, y_count = values.shape
    points_sub = derivative.shape[0]
    x_scale = 4.0 / (points_sub * points_sub)
    rounded = lax.optimization_barrier(values.astype(jnp.bfloat16)).astype(values.dtype)
    along_y = jnp.einsum("pwxk,kj->pwxj", rounded, y_operator.astype(values.dtype), precision=lax.Precision.HIGHEST)
    blocks = values.reshape(parts, wave_count, column_count // points_sub, points_sub, y_count)
    along_x = jnp.einsum("ij,pwsjy->pwsiy", derivative, blocks, precision=lax.Precision.HIGHEST).reshape(values.shape)
    previous = jnp.concatenate([jnp.zeros_like(values[:, :, :1]), values[:, :, :-1]], axis=2)
    first_point = (jnp.arange(column_count) % points_sub == 0).astype(values.dtype)[None, None, :, None]
    jump_term = first_point * (values - previous)
    advect = base_speed[None, None] * (x_scale * along_x + penalty * jump_term)
    sign_factor = jnp.array([1.0, -1.0], values.dtype)[:, None, None, None]
    partner = rounded[::-1]
    return -advect + along_y + sign_factor * coupling[None, :, None, None] * partner - damping[None, :, None, None] * values


def reference(starts_old, y_operator, coarse_inverse, base_speed, damping, coupling):
    derivative = jnp.asarray(cheb_matrix(NP), jnp.float32)
    factor = 1.0 / (1.0 + 2.0 * fine_step * damping)
    inverse_wide = coarse_inverse.astype(jnp.float32)
    ends = []
    last_end = None
    for slice_k in range(SLICES):
        start_now = starts_old[slice_k].astype(jnp.float32)
        middle = start_now + fine_step * slope_of(start_now, y_operator, base_speed, damping, coupling, derivative)
        fine_end = middle + fine_step * slope_of(middle, y_operator, base_speed, damping, coupling, derivative)
        if slice_k == 0:
            end_now = fine_end
        else:
            sent = lax.optimization_barrier(last_end.astype(jnp.bfloat16)).astype(jnp.float32)
            gap = lax.optimization_barrier((sent - start_now).astype(jnp.bfloat16)).astype(jnp.float32)
            mapped = jnp.einsum("ij,pwjy->pwiy", inverse_wide, gap, precision=lax.Precision.HIGHEST)
            end_now = fine_end + factor[None, :, None, None] * mapped
        ends.append(end_now)
        last_end = end_now
    return jnp.stack(ends)
```

```python
import functools

import jax
import jax.numpy as jnp
import numpy as np
from jax import lax
from jax.experimental import pallas as pl
from jax.experimental.pallas import tpu as pltpu
from jax.sharding import PartitionSpec as P

NP = 16
MESH = pl.DeviceIdType.MESH
F32 = jnp.float32
BF16 = jnp.bfloat16

fine_step = 0.25
penalty = 2.0
lanes = 256
pair = 2


def cheb_matrix(points_sub):
    indices = np.arange(points_sub)
    points = -np.cos(np.pi * indices / (points_sub - 1))
    edge_weight = np.where((indices == 0) | (indices == points_sub - 1), 2.0, 1.0)
    sign_table = np.where((indices[:, None] + indices[None, :]) % 2 == 0, 1.0, -1.0)
    identity_table = np.eye(points_sub)
    gap_matrix = points[:, None] - points[None, :] + identity_table
    off_diag = (
        edge_weight[:, None]
        / edge_weight[None, :]
        * sign_table
        / gap_matrix
        * (1.0 - identity_table)
    )
    return off_diag - off_diag.sum(axis=1)[:, None] * identity_table


def advect_matrix(columns):
    derivative = cheb_matrix(NP).astype(np.float32).astype(np.float64)
    table = np.kron(np.eye(columns // NP), derivative) * (4.0 / (NP * NP))
    for row in range(0, columns, NP):
        table[row, row] += penalty
        if row:
            table[row, row - 1] -= penalty
    return fine_step * table


def kernel(
    ny, nz, s_hbm, y_hbm, g_hbm, speed_hbm, a_ref, tail_ref, damp_ref, coup_ref,
    f_hbm, c_hbm,
    s_own, s_next, tails, yop, speed, fine, mid, midb, ax, ay, halo_f, halo_b, halo_in, inflow,
    dsend, lines, cbuf, gmat,
    in_sem, misc_sem, next_send, next_recv, g_send, g_recv, g_local, halo_send, halo_recv,
    line_send, line_recv, x_send, c_send, c_recv, c_local, f_sem,
):
    k = lax.axis_index("cuts")
    j = lax.axis_index("dom")
    v = lax.axis_index("vec")
    y, z = j // nz, lax.rem(j, nz)
    core = lax.rem(k, 2)
    low = k < 2
    dom = ny * nz
    _, waves, cols, ysize = s_hbm.shape
    chunks = ysize // lanes
    half = g_hbm.shape[0]
    quarter = half // 4

    def order(t):
        ty = lax.rem(t, ny)
        tz = lax.rem(t // ny + (nz - 1) * ty, nz)
        return lax.rem(y + ty, ny) * nz + lax.rem(z + tz, nz)

    def remote(src, dst, send, recv, at):
        return pltpu.make_async_remote_copy(
            src_ref=src, dst_ref=dst, send_sem=send, recv_sem=recv, device_id=at, device_id_type=MESH
        )

    load_tails = pltpu.make_async_copy(s_hbm.at[:, :, pl.ds(cols - NP, NP), :], tails, misc_sem.at[0])
    load_y = pltpu.make_async_copy(y_hbm, yop, misc_sem.at[1])
    load_speed = pltpu.make_async_copy(speed_hbm, speed, misc_sem.at[2])
    load_tails.start()
    load_y.start()
    load_speed.start()

    def load_wave(w):
        return pltpu.make_async_copy(s_hbm.at[:, w], s_own.at[w], in_sem.at[w])

    def start_wave(t, carry):
        load_wave(order(t)).start()
        return carry

    lax.fori_loop(0, waves, start_wave, 0)

    own_at = pl.multiple_of(v * half, half)
    other_at = pl.multiple_of((1 - v) * half, half)
    load_g = pltpu.make_async_copy(g_hbm, gmat.at[pl.ds(own_at, half)], g_local)
    load_g.start()

    def send_g(side):
        rows = pl.multiple_of((2 * side + core) * quarter, quarter)
        at = (k if side == 0 else lax.rem(k + 2, 4), j, 1 - v)
        return remote(
            g_hbm.at[pl.ds(rows, quarter)],
            gmat.at[pl.ds(pl.multiple_of(own_at + rows, quarter), quarter)],
            g_send.at[side], g_recv.at[side], at,
        )

    def pass_g(side):
        rows = pl.multiple_of(other_at + (2 * side + core) * quarter, quarter)
        part = gmat.at[pl.ds(rows, quarter)]
        return remote(part, part, g_send.at[2 + side], g_recv.at[2 + side], (k + 1 - 2 * core, j, v))

    send_g(0).start()
    send_g(1).start()

    def send_next(i, w, at):
        return remote(
            s_hbm.at[:, w, :, pl.ds(i * lanes, lanes)], s_next.at[i, w], next_send, next_recv.at[i, w], at
        )

    @pl.when(k > 0)
    def _():
        for i in range(chunks):

            def start_next(t, carry):
                send_next(i, order(t), (k - 1, j, v)).start()
                return carry

            lax.fori_loop(0, waves, start_next, 0)

    load_tails.wait()
    load_y.wait()
    load_speed.wait()
    yop[...] = (yop[...].astype(F32) * fine_step).astype(BF16)

    def gather_tail(w, carry):
        for p in range(2):
            rows = tails[p, w].astype(F32)
            at = pl.ds(p * waves + w, 1)
            halo_f[0, at, :] = rows[NP - 1 : NP, :]
            halo_f[1, at, :] = jnp.sum(rows * tail_ref[:, 0:1], axis=0, keepdims=True)
        return carry

    lax.fori_loop(0, waves, gather_tail, 0)
    halo_b[0] = halo_f[0].astype(BF16)
    halo_f[2] = jnp.dot(halo_b[0], yop[...], preferred_element_type=F32)

    def middle_tail(w, carry):
        keep = 1.0 - fine_step * damp_ref[w]
        cross = fine_step * coup_ref[w]
        for p in range(2):
            at = pl.ds(p * waves + w, 1)
            other = pl.ds((1 - p) * waves + w, 1)
            swap = cross if p == 0 else -cross
            halo_f[3, at, :] = (
                keep * halo_f[0, at, :]
                + halo_f[2, at, :]
                + swap * halo_f[0, other, :]
                - speed[cols - 1 : cols, :] * halo_f[1, at, :]
            )
        return carry

    lax.fori_loop(0, waves, middle_tail, 0)
    halo_b[1] = halo_f[3].astype(BF16)

    def send_halo():
        return remote(halo_b, halo_in, halo_send, halo_recv, (k, j + 1, v))

    @pl.when(j < dom - 1)
    def _():
        send_halo().start()

    @pl.when(j > 0)
    def _():
        remote(halo_b, halo_in, halo_send, halo_recv, (k, j - 1, v)).wait_recv()
        inflow[...] = (fine_step * penalty) * halo_in[...].astype(F32)

    @pl.when(j == 0)
    def _():
        inflow[...] = jnp.zeros_like(inflow)

    first = lax.broadcasted_iota(jnp.int32, (NP, ysize), 0) == 0

    def slope_products(values):
        flat = jnp.concatenate([x.reshape(2 * cols, ysize) for x in values], axis=0)
        for at in range(0, ysize, lanes):
            ay[:, at : at + lanes] = jnp.dot(flat, yop[:, at : at + lanes], preferred_element_type=F32)
        for q, x in enumerate(values):
            for p in range(2):
                ax[q, p] = jnp.dot(a_ref[...], x[p], preferred_element_type=F32)

    def combine(q, w, stage, own, partner, put):
        keep = 1.0 - fine_step * damp_ref[w]
        cross = fine_step * coup_ref[w]
        for p in range(2):
            swap = cross if p == 0 else -cross
            for r in range(0, cols, NP):
                along_x = ax[q, p, r : r + NP, :]
                if r == 0:
                    row = inflow[stage, pl.ds(p * waves + w, 1), :]
                    along_x = along_x - jnp.where(first, row, 0.0)
                at = (2 * q + p) * cols + r
                put(
                    p,
                    r,
                    keep * own(p, r)
                    + ay[at : at + NP, :]
                    + swap * partner(1 - p, r)
                    - speed[r : r + NP, :] * along_x,
                )

    def emit(i, w):
        @pl.when(k < 3)
        def _():
            send_next(i, w, (k + 1, j, v)).wait_recv()
            for p in range(2):
                gap = (fine[w, p, :, i * lanes : (i + 1) * lanes] - s_next[i, w, p].astype(F32)).astype(BF16)
                target = lines.at[core, i, pl.ds(pl.multiple_of(j * cols, cols), cols)]
                mine = (w == j) & (core == p)

                @pl.when(mine)
                def _():
                    target[...] = gap

                @pl.when(jnp.logical_not(mine))
                def _():
                    dsend[i, w, p] = gap
                    remote(
                        dsend.at[i, w, p], target, line_send.at[p], line_recv.at[core, i],
                        (k - core + p, w, v),
                    ).start()

    def store_fine(w):
        return pltpu.make_async_copy(fine.at[w], f_hbm.at[:, w], f_sem)

    def fine_waves(t, carry):
        ws = [order(t * pair + q) for q in range(pair)]
        for w in ws:
            load_wave(w).wait()
        slope_products([s_own[w] for w in ws])
        for q, w in enumerate(ws):

            def put_middle(p, r, value):
                mid[q, p, r : r + NP, :] = value
                midb[q, p, r : r + NP, :] = value.astype(BF16)

            def start_rows(p, r):
                return s_own[w, p, r : r + NP, :].astype(F32)

            combine(q, w, 0, start_rows, start_rows, put_middle)
        slope_products([midb[q] for q in range(pair)])
        for q, w in enumerate(ws):

            def put_fine(p, r, value):
                fine[w, p, r : r + NP, :] = value

            combine(
                q, w, 1,
                lambda p, r: mid[q, p, r : r + NP, :],
                lambda p, r: midb[q, p, r : r + NP, :].astype(F32),
                put_fine,
            )
            store_fine(w).start()

            @pl.when(k != 1)
            def _():
                emit(0, w)

        return carry

    lax.fori_loop(0, waves // pair, fine_waves, 0)

    def emit_chunk(i):
        def step(t, carry):
            emit(i, order(t))
            return carry

        lax.fori_loop(0, waves, step, 0)

    @pl.when(k == 1)
    def _():
        emit_chunk(0)

    for side in range(2):
        send_g(side).wait_recv()
        pass_g(side).start()
    for i in range(1, chunks):
        emit_chunk(i)
    load_g.wait()
    for side in range(2):
        pass_g(side).wait_recv()

    gain = 1.0 / (1.0 + 2.0 * fine_step * jnp.full((1, lanes), damp_ref[j], F32))
    group = nz * cols

    def wait_lines(b, i, less):
        part = lines.at[b, i, pl.ds(0, (dom - less) * cols)]
        remote(part, part, line_send.at[b], line_recv.at[b, i], (k, j, v)).wait_recv()

    def piece_of(source, i, at, to, queue):
        rows = pl.ds(pl.multiple_of(at * cols, cols), cols)
        spot = c_hbm.at[core, j, :, pl.ds(i * lanes, lanes)]
        return remote(source.at[rows], spot, c_send.at[queue], c_recv.at[core, i], (to, at, v))

    def own_piece(source, i, at):
        rows = pl.ds(pl.multiple_of(at * cols, cols), cols)
        return pltpu.make_async_copy(source.at[rows], c_hbm.at[core, j, :, pl.ds(i * lanes, lanes)], c_local.at[i])

    def send_pieces(source, i, block, to, queue):
        def step(t, carry):
            at = block * nz + lax.rem(z + t, nz)
            mine = (at == j) & (k == to)

            @pl.when(mine)
            def _():
                own_piece(source, i, at).start()

            @pl.when(jnp.logical_not(mine))
            def _():
                piece_of(source, i, at, to, queue).start()

            return carry

        lax.fori_loop(0, nz, step, 0)

    def product(source, out, after):
        def step(t, carry):
            block = lax.rem(y + t, ny)
            rows = pl.ds(pl.multiple_of(block * group, group), group)
            total = jnp.dot(gmat[rows, :], source[...], preferred_element_type=F32)
            out[rows, :] = (gain * total).astype(BF16)
            after(block, rows)
            return carry

        lax.fori_loop(0, ny, step, 0)

    def add_lines(target, term):
        def step(t, carry):
            rows = pl.ds(pl.multiple_of(t * cols, cols), cols)
            target[rows, :] = (target[rows, :].astype(F32) + term[rows, :].astype(F32)).astype(BF16)
            return carry

        lax.fori_loop(0, dom, step, 0)

    def across(i, rows):
        return remote(cbuf.at[1, i, rows], lines.at[1, i, rows], x_send, line_recv.at[1, i], (k + 2, j, v))

    for i in range(chunks):

        @pl.when(core == 0)
        def _():
            wait_lines(0, i, 1)

        @pl.when(core == 1)
        def _():
            wait_lines(0, i, 0)

        @pl.when(low)
        def _():
            product(lines.at[0, i], cbuf.at[0, i], lambda block, rows: send_pieces(cbuf.at[0, i], i, block, 1, 0))

            @pl.when(core == 0)
            def _():
                wait_lines(1, i, 0)

            @pl.when(core == 1)
            def _():
                wait_lines(1, i, 1)

            add_lines(lines.at[1, i], cbuf.at[0, i])
            product(lines.at[1, i], cbuf.at[1, i], lambda block, rows: across(i, rows).start())

        @pl.when(jnp.logical_not(low))
        def _():
            wait_lines(1, i, 0)

            def forward(t, carry):
                send_pieces(lines.at[1, i], i, lax.rem(y + t, ny), 2, 1)
                return carry

            lax.fori_loop(0, ny, forward, 0)
            add_lines(lines.at[0, i], lines.at[1, i])
            product(lines.at[0, i], cbuf.at[0, i], lambda block, rows: send_pieces(cbuf.at[0, i], i, block, 3, 0))

    def done(part, send, recv):
        return remote(part, part, send, recv, (k, j, v))

    def block_of(less):
        return cbuf.at[0, :, pl.ds(0, (dom - less) * cols)]

    def line_of(less):
        return cbuf.at[0, 0, pl.ds(0, (dom - less) * cols)]

    for p in range(2):

        @pl.when(core == p)
        def _():
            @pl.when(k > 0)
            def _():
                for i in range(chunks):
                    done(line_of(1), c_send.at[0], c_recv.at[p, i]).wait_recv()
                    done(line_of(0), c_send.at[0], c_recv.at[1 - p, i]).wait_recv()
                    own_piece(cbuf.at[0, i], i, 0).wait()

            @pl.when(k < 3)
            def _():
                done(block_of(1), line_send.at[p], c_recv.at[0, 0]).wait_send()
                done(block_of(0), line_send.at[1 - p], c_recv.at[0, 0]).wait_send()

            done(block_of(p), c_send.at[0], c_recv.at[0, 0]).wait_send()

            @pl.when(jnp.logical_not(low))
            def _():
                done(block_of(1 - p), c_send.at[1], c_recv.at[0, 0]).wait_send()

    @pl.when(k > 0)
    def _():
        done(s_next, next_send, next_recv.at[0, 0]).wait_send()

    @pl.when(low)
    def _():
        done(block_of(0), x_send, c_recv.at[0, 0]).wait_send()

    @pl.when(j < dom - 1)
    def _():
        send_halo().wait_send()

    for side in range(2):
        send_g(side).wait_send()
        pass_g(side).wait_send()
    pltpu.make_async_copy(f_hbm, f_hbm, f_sem).wait()


def call(torus, state, y_operator, coarse_inverse, base_speed, damping, coupling):
    ny, nz = torus
    dom = ny * nz
    parts, waves, cols, ysize = state.shape
    assert parts == 2 and waves == dom and ysize % lanes == 0 and waves % pair == 0
    chunks = ysize // lanes
    length = dom * cols
    table = advect_matrix(cols)
    a_mat = jnp.asarray(table, BF16)
    tail = jnp.broadcast_to(jnp.asarray(table[-1, -NP:], F32)[:, None], (NP, 128))
    anywhere = pl.BlockSpec(memory_space=pl.ANY)
    vmem = pl.BlockSpec(memory_space=pltpu.VMEM)
    smem = pl.BlockSpec(memory_space=pltpu.SMEM)
    dma = pltpu.SemaphoreType.DMA
    return pl.pallas_call(
        functools.partial(kernel, ny, nz),
        out_shape=(
            jax.ShapeDtypeStruct(state.shape, F32),
            jax.ShapeDtypeStruct(state.shape, BF16),
        ),
        in_specs=[anywhere] * 4 + [vmem] * 2 + [smem] * 2,
        out_specs=(anywhere, anywhere),
        scratch_shapes=[
            pltpu.VMEM((waves, 2, cols, ysize), BF16),
            pltpu.VMEM((chunks, waves, 2, cols, lanes), BF16),
            pltpu.VMEM((2, waves, NP, ysize), BF16),
            pltpu.VMEM((ysize, ysize), BF16),
            pltpu.VMEM((cols, ysize), F32),
            pltpu.VMEM((waves, 2, cols, ysize), F32),
            pltpu.VMEM((pair, 2, cols, ysize), F32),
            pltpu.VMEM((pair, 2, cols, ysize), BF16),
            pltpu.VMEM((pair, 2, cols, ysize), F32),
            pltpu.VMEM((pair * 2 * cols, ysize), F32),
            pltpu.VMEM((4, 2 * waves, ysize), F32),
            pltpu.VMEM((2, 2 * waves, ysize), BF16),
            pltpu.VMEM((2, 2 * waves, ysize), BF16),
            pltpu.VMEM((2, 2 * waves, ysize), F32),
            pltpu.VMEM((chunks, waves, 2, cols, lanes), BF16),
            pltpu.VMEM((2, chunks, length, lanes), BF16),
            pltpu.VMEM((2, chunks, length, lanes), BF16),
            pltpu.VMEM((length, length), BF16),
            dma((waves,)),
            dma((3,)),
            dma,
            dma((chunks, waves)),
            dma((4,)),
            dma((4,)),
            dma,
            dma,
            dma,
            dma((2,)),
            dma((2, chunks)),
            dma,
            dma((2,)),
            dma((2, chunks)),
            dma((chunks,)),
            dma,
        ],
        compiler_params=pltpu.CompilerParams(has_side_effects=True, vmem_limit_bytes=62 * 2**20),
        name="parareal",
    )(state, y_operator, coarse_inverse, base_speed, a_mat, tail, damping, coupling)


def local(torus, starts_old, y_operator, coarse_inverse, base_speed, damping, coupling):
    fine_end, change = call(torus, starts_old[0], y_operator, coarse_inverse, base_speed, damping, coupling)
    is_leader = lax.axis_index("cuts") == 0
    return jnp.where(is_leader, fine_end, fine_end + change.astype(F32))[None]


def solution(mesh):
    dom = mesh.shape["dom"]
    torus = (4, 4) if dom == 16 else (1, dom)
    in_specs = (
        P("cuts", None, "vec", "dom", None),
        P(),
        P("vec", None),
        P("dom", None),
        P("vec"),
        P("vec"),
    )
    out_specs = P("cuts", None, "vec", "dom", None)
    return jax.shard_map(
        functools.partial(local, torus), mesh=mesh, in_specs=in_specs, out_specs=out_specs, check_vma=False
    )
```

```python
import functools

import jax
import jax.numpy as jnp
import numpy as np
from jax import lax
from jax.experimental import pallas as pl
from jax.experimental.pallas import tpu as pltpu
from jax.sharding import PartitionSpec as P

NP = 16
MESH = pl.DeviceIdType.MESH
F32 = jnp.float32
BF16 = jnp.bfloat16

fine_step = 0.25
penalty = 2.0
lanes = 128
block = 256
pair = 2


def cheb_matrix(points_sub):
    indices = np.arange(points_sub)
    points = -np.cos(np.pi * indices / (points_sub - 1))
    edge_weight = np.where((indices == 0) | (indices == points_sub - 1), 2.0, 1.0)
    sign_table = np.where((indices[:, None] + indices[None, :]) % 2 == 0, 1.0, -1.0)
    identity_table = np.eye(points_sub)
    gap_matrix = points[:, None] - points[None, :] + identity_table
    off_diag = (
        edge_weight[:, None]
        / edge_weight[None, :]
        * sign_table
        / gap_matrix
        * (1.0 - identity_table)
    )
    return off_diag - off_diag.sum(axis=1)[:, None] * identity_table


def advect_matrix(columns):
    derivative = cheb_matrix(NP).astype(np.float32).astype(np.float64)
    table = np.kron(np.eye(columns // NP), derivative) * (4.0 / (NP * NP))
    for row in range(0, columns, NP):
        table[row, row] += penalty
        if row:
            table[row, row - 1] -= penalty
    return fine_step * table


def kernel(
    ny, nz, s_hbm, y_hbm, g_hbm, speed_hbm, a_ref, tail_ref, damp_ref, coup_ref,
    fine,
    s_own, s_next, tails, yop, speed, mid, midb, ax, ay, halo_f, halo_b, halo_in, inflow,
    dsend, lines, cbuf, gmat, c_in,
    in_sem, misc_sem, next_send, next_recv, g_send, g_recv, g_local, halo_send, halo_recv,
    line_send, line_recv, x_send, c_send, c_recv,
):
    k = lax.axis_index("cuts")
    j = lax.axis_index("dom")
    v = lax.axis_index("vec")
    y, z = j // nz, lax.rem(j, nz)
    core = lax.rem(k, 2)
    low = k < 2
    dom = ny * nz
    _, waves, cols, ysize = s_hbm.shape
    chunks = ysize // lanes
    half = g_hbm.shape[0]
    ahead = chunks // 2
    quarter = half // 4

    def order(t):
        ty = lax.rem(t, ny)
        tz = lax.rem(t // ny + (nz - 1) * ty, nz)
        return lax.rem(y + ty, ny) * nz + lax.rem(z + tz, nz)

    def remote(src, dst, send, recv, at):
        return pltpu.make_async_remote_copy(
            src_ref=src, dst_ref=dst, send_sem=send, recv_sem=recv, device_id=at, device_id_type=MESH
        )

    twin = (k + 1 - 2 * core, j, v)
    barrier = pltpu.get_barrier_semaphore()

    def greet(at):
        pl.semaphore_signal(barrier, inc=1, device_id=at, device_id_type=MESH)

    def greet_dom(t, carry):
        at = lax.rem(j + t, dom)
        greet((k, at, v))
        greet((k + 1 - 2 * core, at, v))
        return carry

    lax.fori_loop(1, dom, greet_dom, 0)
    greet(twin)
    for there in (k, twin[0]):
        greet((lax.rem(there + 2, 4), j, v))
    greet((k, j, 1 - v))
    greet((lax.rem(k + 2, 4), j, 1 - v))

    load_tails = pltpu.make_async_copy(s_hbm.at[:, :, pl.ds(cols - NP, NP), :], tails, misc_sem.at[0])
    load_y = pltpu.make_async_copy(y_hbm, yop, misc_sem.at[1])
    load_speed = pltpu.make_async_copy(speed_hbm, speed, misc_sem.at[2])
    load_tails.start()
    load_y.start()
    load_speed.start()

    def load_wave(w):
        return pltpu.make_async_copy(s_hbm.at[:, w], s_own.at[w], in_sem.at[w])

    def start_wave(t, carry):
        load_wave(order(t)).start()
        return carry

    lax.fori_loop(0, waves, start_wave, 0)

    half_rows = half // 2
    own_at = pl.multiple_of(v * half, half)
    other_at = pl.multiple_of((1 - v) * half, half)
    load_g = pltpu.make_async_copy(g_hbm, gmat.at[pl.ds(own_at, half)], g_local)
    load_g.start()

    def send_g(to, queue):
        rows = pl.multiple_of(core * half_rows, half_rows)
        return remote(
            g_hbm.at[pl.ds(rows, half_rows)],
            gmat.at[pl.ds(pl.multiple_of(own_at + rows, half_rows), half_rows)],
            g_send.at[queue], g_recv.at[0], (to, j, 1 - v),
        )

    def g_twin():
        part = gmat.at[pl.ds(pl.multiple_of(other_at + core * half_rows, half_rows), half_rows)]
        return remote(part, part, g_send.at[2], g_recv.at[1], twin)

    def send_next(i, w, at):
        return remote(
            s_hbm.at[:, w, :, pl.ds(i * lanes, lanes)], s_next.at[i, w], next_send, next_recv.at[i, w], at
        )

    load_tails.wait()
    load_y.wait()
    load_speed.wait()
    yop[...] = (yop[...].astype(F32) * fine_step).astype(BF16)

    def gather_tail(w, carry):
        for p in range(2):
            rows = tails[p, w].astype(F32)
            at = pl.ds(p * waves + w, 1)
            halo_f[0, at, :] = rows[NP - 1 : NP, :]
            halo_f[1, at, :] = jnp.sum(rows * tail_ref[:, 0:1], axis=0, keepdims=True)
        return carry

    lax.fori_loop(0, waves, gather_tail, 0)
    halo_b[0] = halo_f[0].astype(BF16)
    halo_f[2] = jnp.dot(halo_b[0], yop[...], preferred_element_type=F32)

    def middle_tail(w, carry):
        keep = 1.0 - fine_step * damp_ref[w]
        cross = fine_step * coup_ref[w]
        for p in range(2):
            at = pl.ds(p * waves + w, 1)
            other = pl.ds((1 - p) * waves + w, 1)
            swap = cross if p == 0 else -cross
            halo_f[3, at, :] = (
                keep * halo_f[0, at, :]
                + halo_f[2, at, :]
                + swap * halo_f[0, other, :]
                - speed[cols - 1 : cols, :] * halo_f[1, at, :]
            )
        return carry

    lax.fori_loop(0, waves, middle_tail, 0)
    halo_b[1] = halo_f[3].astype(BF16)

    def send_halo():
        return remote(halo_b, halo_in, halo_send, halo_recv, (k, j + 1, v))

    pl.semaphore_wait(barrier, 2 * dom - 1 + 4)

    @pl.when(j < dom - 1)
    def _():
        send_halo().start()

    @pl.when(k > 0)
    def _():
        for i in range(chunks):

            def start_next(t, carry):
                send_next(i, order(t), (k - 1, j, v)).start()
                return carry

            lax.fori_loop(0, waves, start_next, 0)

    @pl.when(low)
    def _():
        send_g(k, 0).start()
        send_g(k + 2, 1).start()

    @pl.when(j > 0)
    def _():
        remote(halo_b, halo_in, halo_send, halo_recv, (k, j - 1, v)).wait_recv()
        inflow[...] = (fine_step * penalty) * halo_in[...].astype(F32)

    @pl.when(j == 0)
    def _():
        inflow[...] = jnp.zeros_like(inflow)

    first = lax.broadcasted_iota(jnp.int32, (NP, ysize), 0) == 0

    def slope_products(values):
        flat = jnp.concatenate([x.reshape(2 * cols, ysize) for x in values], axis=0)
        for at in range(0, ysize, block):
            ay[:, at : at + block] = jnp.dot(flat, yop[:, at : at + block], preferred_element_type=F32)
        for q, x in enumerate(values):
            for p in range(2):
                ax[q, p] = jnp.dot(a_ref[...], x[p], preferred_element_type=F32)

    def combine(q, w, stage, own, partner, put):
        keep = 1.0 - fine_step * damp_ref[w]
        cross = fine_step * coup_ref[w]
        for p in range(2):
            swap = cross if p == 0 else -cross
            for r in range(0, cols, NP):
                along_x = ax[q, p, r : r + NP, :]
                if r == 0:
                    row = inflow[stage, pl.ds(p * waves + w, 1), :]
                    along_x = along_x - jnp.where(first, row, 0.0)
                at = (2 * q + p) * cols + r
                put(
                    p,
                    r,
                    keep * own(p, r)
                    + ay[at : at + NP, :]
                    + swap * partner(1 - p, r)
                    - speed[r : r + NP, :] * along_x,
                )

    def emit(i, w):
        @pl.when(k < 3)
        def _():
            send_next(i, w, (k + 1, j, v)).wait_recv()
            for p in range(2):
                gap = (fine[p, w, :, i * lanes : (i + 1) * lanes] - s_next[i, w, p].astype(F32)).astype(BF16)
                target = lines.at[core, i, pl.ds(pl.multiple_of(j * cols, cols), cols)]
                mine = (w == j) & (core == p)

                @pl.when(mine)
                def _():
                    target[...] = gap

                @pl.when(jnp.logical_not(mine))
                def _():
                    dsend[i, w, p] = gap
                    remote(
                        dsend.at[i, w, p], target, line_send.at[p], line_recv.at[core, i],
                        (k - core + p, w, v),
                    ).start()

    def fine_waves(t, carry):
        ws = [order(t * pair + q) for q in range(pair)]
        for w in ws:
            load_wave(w).wait()
        slope_products([s_own[w] for w in ws])
        for q, w in enumerate(ws):

            def put_middle(p, r, value):
                mid[q, p, r : r + NP, :] = value
                midb[q, p, r : r + NP, :] = value.astype(BF16)

            def start_rows(p, r):
                return s_own[w, p, r : r + NP, :].astype(F32)

            combine(q, w, 0, start_rows, start_rows, put_middle)
        slope_products([midb[q] for q in range(pair)])
        for q, w in enumerate(ws):

            def put_fine(p, r, value):
                fine[p, w, r : r + NP, :] = value

            combine(
                q, w, 1,
                lambda p, r: mid[q, p, r : r + NP, :],
                lambda p, r: midb[q, p, r : r + NP, :].astype(F32),
                put_fine,
            )

            @pl.when(k != 1)
            def _():
                for i in range(ahead):
                    emit(i, w)

        return carry

    lax.fori_loop(0, waves // pair, fine_waves, 0)

    def emit_chunk(i):
        def step(t, carry):
            emit(i, order(t))
            return carry

        lax.fori_loop(0, waves, step, 0)

    @pl.when(k == 1)
    def _():
        for i in range(ahead):
            emit_chunk(i)

    @pl.when(k != 1)
    def _():
        for i in range(ahead, chunks):
            emit_chunk(i)

    send_g(k, 0).wait_recv()
    g_twin().start()
    load_g.wait()
    g_twin().wait_recv()

    gain = 1.0 / (1.0 + 2.0 * fine_step * jnp.full((1, lanes), damp_ref[j], F32))
    group = nz * cols

    def wait_lines(b, i, less):
        part = lines.at[b, i, pl.ds(0, (dom - less) * cols)]
        remote(part, part, line_send.at[b], line_recv.at[b, i], (k, j, v)).wait_recv()

    def spot(i, w, p):
        return c_in.at[p, w, :, pl.ds(i * lanes, lanes)]

    def send_pieces(source, i, block, to, queue):
        def step(t, carry):
            at = block * nz + lax.rem(z + t, nz)
            rows = pl.ds(pl.multiple_of(at * cols, cols), cols)
            mine = (at == j) & (k == to)

            @pl.when(mine)
            def _():
                c_in[core, j, :, i * lanes : (i + 1) * lanes] = source[rows, :]

            @pl.when(jnp.logical_not(mine))
            def _():
                remote(
                    source.at[rows], spot(i, j, core), c_send.at[queue], c_recv.at[core, i], (to, at, v)
                ).start()

            return carry

        lax.fori_loop(0, nz, step, 0)

    def product(source, out, after):
        def step(t, carry):
            block = lax.rem(y + t, ny)
            rows = pl.ds(pl.multiple_of(block * group, group), group)
            total = jnp.dot(gmat[rows, :], source[...], preferred_element_type=F32)
            out[rows, :] = (gain * total).astype(BF16)
            after(block, rows)
            return carry

        lax.fori_loop(0, ny, step, 0)

    def add_lines(target, term):
        def step(t, carry):
            rows = pl.ds(pl.multiple_of(t * cols, cols), cols)
            target[rows, :] = (target[rows, :].astype(F32) + term[rows, :].astype(F32)).astype(BF16)
            return carry

        lax.fori_loop(0, dom, step, 0)

    def across(i, rows):
        return remote(cbuf.at[1, i, rows], lines.at[1, i, rows], x_send, line_recv.at[1, i], (k + 2, j, v))

    def wait_pieces(p, i, less):
        part = cbuf.at[0, 0, pl.ds(0, (dom - less) * cols)]
        remote(part, part, c_send.at[0], c_recv.at[p, i], (k, j, v)).wait_recv()

    def wait_both(b, i):
        @pl.when(core == b)
        def _():
            wait_lines(b, i, 1)

        @pl.when(core != b)
        def _():
            wait_lines(b, i, 0)

    for i in range(chunks):
        wait_both(0, i)

        @pl.when(low)
        def _():
            product(lines.at[0, i], cbuf.at[0, i], lambda block, rows: None)

            wait_both(1, i)
            add_lines(lines.at[1, i], cbuf.at[0, i])
            product(lines.at[1, i], cbuf.at[1, i], lambda block, rows: across(i, rows).start())

            if i + ahead < chunks:

                @pl.when(k == 1)
                def _():
                    emit_chunk(i + ahead)

        @pl.when(jnp.logical_not(low))
        def _():
            wait_lines(1, i, 0)

            def forward(t, carry):
                send_pieces(lines.at[1, i], i, lax.rem(y + t, ny), 2, 1)
                return carry

            lax.fori_loop(0, ny, forward, 0)
            add_lines(lines.at[0, i], lines.at[1, i])
            product(lines.at[0, i], cbuf.at[0, i], lambda block, rows: send_pieces(cbuf.at[0, i], i, block, 3, 0))

    @pl.when(low)
    def _():
        for i in range(chunks):

            def give(t, carry):
                send_pieces(cbuf.at[0, i], i, lax.rem(y + t, ny), 1, 0)
                return carry

            lax.fori_loop(0, ny, give, 0)

    @pl.when(k > 0)
    def _():
        for i in range(chunks):
            for p in range(2):

                @pl.when(core == p)
                def _():
                    wait_pieces(p, i, 1)

                @pl.when(core != p)
                def _():
                    wait_pieces(p, i, 0)

            at = slice(i * lanes, (i + 1) * lanes)

            def add_change(w, carry):
                for p in range(2):
                    fine[p, w, :, at] = fine[p, w, :, at] + c_in[p, w, :, at].astype(F32)
                return carry

            lax.fori_loop(0, waves, add_change, 0)

    def done(part, send, recv):
        return remote(part, part, send, recv, (k, j, v))

    def block_of(less):
        return cbuf.at[0, :, pl.ds(0, (dom - less) * cols)]

    for p in range(2):

        @pl.when(core == p)
        def _():
            @pl.when(k < 3)
            def _():
                done(block_of(1), line_send.at[p], c_recv.at[0, 0]).wait_send()
                done(block_of(0), line_send.at[1 - p], c_recv.at[0, 0]).wait_send()

            done(block_of(p), c_send.at[0], c_recv.at[0, 0]).wait_send()

            @pl.when(jnp.logical_not(low))
            def _():
                done(block_of(1 - p), c_send.at[1], c_recv.at[0, 0]).wait_send()

    @pl.when(k > 0)
    def _():
        done(s_next, next_send, next_recv.at[0, 0]).wait_send()

    @pl.when(low)
    def _():
        done(block_of(0), x_send, c_recv.at[0, 0]).wait_send()

    @pl.when(j < dom - 1)
    def _():
        send_halo().wait_send()

    @pl.when(low)
    def _():
        send_g(k, 0).wait_send()
        send_g(k + 2, 1).wait_send()

    g_twin().wait_send()


def call(torus, state, y_operator, coarse_inverse, base_speed, damping, coupling):
    ny, nz = torus
    dom = ny * nz
    parts, waves, cols, ysize = state.shape
    assert parts == 2 and waves == dom and ysize % lanes == 0 and waves % pair == 0
    chunks = ysize // lanes
    length = dom * cols
    table = advect_matrix(cols)
    a_mat = jnp.asarray(table, BF16)
    tail = jnp.asarray(np.repeat(table[-1, -NP:, None], 128, axis=1), F32)
    anywhere = pl.BlockSpec(memory_space=pl.ANY)
    vmem = pl.BlockSpec(memory_space=pltpu.VMEM)
    smem = pl.BlockSpec(memory_space=pltpu.SMEM)
    dma = pltpu.SemaphoreType.DMA
    return pl.pallas_call(
        functools.partial(kernel, ny, nz),
        out_shape=pltpu.VMEM(state.shape, F32),
        in_specs=[anywhere] * 4 + [vmem] * 2 + [smem] * 2,
        out_specs=vmem,
        scratch_shapes=[
            pltpu.VMEM((waves, 2, cols, ysize), BF16),
            pltpu.VMEM((chunks, waves, 2, cols, lanes), BF16),
            pltpu.VMEM((2, waves, NP, ysize), BF16),
            pltpu.VMEM((ysize, ysize), BF16),
            pltpu.VMEM((cols, ysize), F32),
            pltpu.VMEM((pair, 2, cols, ysize), F32),
            pltpu.VMEM((pair, 2, cols, ysize), BF16),
            pltpu.VMEM((pair, 2, cols, ysize), F32),
            pltpu.VMEM((pair * 2 * cols, ysize), F32),
            pltpu.VMEM((4, 2 * waves, ysize), F32),
            pltpu.VMEM((2, 2 * waves, ysize), BF16),
            pltpu.VMEM((2, 2 * waves, ysize), BF16),
            pltpu.VMEM((2, 2 * waves, ysize), F32),
            pltpu.VMEM((chunks, waves, 2, cols, lanes), BF16),
            pltpu.VMEM((2, chunks, length, lanes), BF16),
            pltpu.VMEM((2, chunks, length, lanes), BF16),
            pltpu.VMEM((length, length), BF16),
            pltpu.VMEM((2, waves, cols, ysize), BF16),
            dma((waves,)),
            dma((3,)),
            dma,
            dma((chunks, waves)),
            dma((3,)),
            dma((2,)),
            dma,
            dma,
            dma,
            dma((2,)),
            dma((2, chunks)),
            dma,
            dma((2,)),
            dma((2, chunks)),
        ],
        compiler_params=pltpu.CompilerParams(collective_id=0, has_side_effects=True, vmem_limit_bytes=50 * 2**20),
        name="parareal",
    )(state, y_operator, coarse_inverse, base_speed, a_mat, tail, damping, coupling)


def local(torus, starts_old, y_operator, coarse_inverse, base_speed, damping, coupling):
    return call(torus, starts_old[0], y_operator, coarse_inverse, base_speed, damping, coupling)[None]


def solution(mesh):
    dom = mesh.shape["dom"]
    torus = (4, 4) if dom == 16 else (1, dom)
    in_specs = (
        P("cuts", None, "vec", "dom", None),
        P(),
        P("vec", None),
        P("dom", None),
        P("vec"),
        P("vec"),
    )
    out_specs = P("cuts", None, "vec", "dom", None)
    return jax.shard_map(
        functools.partial(local, torus), mesh=mesh, in_specs=in_specs, out_specs=out_specs, check_vma=False
    )
```

```python
import functools

import jax
import jax.numpy as jnp
import numpy as np
from jax import lax
from jax.experimental import pallas as pl
from jax.experimental.pallas import tpu as pltpu
from jax.sharding import PartitionSpec as P

NP = 16
MESH = pl.DeviceIdType.MESH
F32 = jnp.float32
BF16 = jnp.bfloat16

fine_step = 0.25
penalty = 2.0
lanes = 128
block = 256
pair = 2


def cheb_matrix(points_sub):
    indices = np.arange(points_sub)
    points = -np.cos(np.pi * indices / (points_sub - 1))
    edge_weight = np.where((indices == 0) | (indices == points_sub - 1), 2.0, 1.0)
    sign_table = np.where((indices[:, None] + indices[None, :]) % 2 == 0, 1.0, -1.0)
    identity_table = np.eye(points_sub)
    gap_matrix = points[:, None] - points[None, :] + identity_table
    off_diag = (
        edge_weight[:, None]
        / edge_weight[None, :]
        * sign_table
        / gap_matrix
        * (1.0 - identity_table)
    )
    return off_diag - off_diag.sum(axis=1)[:, None] * identity_table


def advect_matrix(columns):
    derivative = cheb_matrix(NP).astype(np.float32).astype(np.float64)
    table = np.kron(np.eye(columns // NP), derivative) * (4.0 / (NP * NP))
    for row in range(0, columns, NP):
        table[row, row] += penalty
        if row:
            table[row, row - 1] -= penalty
    return fine_step * table


def kernel(
    ny, nz, s_hbm, y_hbm, g_hbm, speed_hbm, a_ref, tail_ref, damp_ref, coup_ref,
    fine,
    s_own, s_next, tails, yop, speed, mid, midb, ax, ay, halo_f, halo_b, halo_in, inflow,
    dsend, lines, cbuf, gmat, c_in,
    in_sem, misc_sem, next_send, next_recv, g_send, g_recv, g_local, halo_send, halo_recv,
    line_send, line_recv, x_send, x_recv, c_send, c_recv,
):
    k = lax.axis_index("cuts")
    j = lax.axis_index("dom")
    v = lax.axis_index("vec")
    y, z = j // nz, lax.rem(j, nz)
    core = lax.rem(k, 2)
    low = k < 2
    dom = ny * nz
    _, waves, cols, ysize = s_hbm.shape
    chunks = ysize // lanes
    half = g_hbm.shape[0]
    ahead = chunks // 2
    quarter = half // 4

    def order(t):
        ty = lax.rem(t, ny)
        tz = lax.rem(t // ny + (nz - 1) * ty, nz)
        return lax.rem(y + ty, ny) * nz + lax.rem(z + tz, nz)

    def remote(src, dst, send, recv, at):
        return pltpu.make_async_remote_copy(
            src_ref=src, dst_ref=dst, send_sem=send, recv_sem=recv, device_id=at, device_id_type=MESH
        )

    twin = (k + 1 - 2 * core, j, v)
    barrier = pltpu.get_barrier_semaphore()

    def greet(at):
        pl.semaphore_signal(barrier, inc=1, device_id=at, device_id_type=MESH)

    def greet_dom(t, carry):
        at = lax.rem(j + t, dom)
        greet((k, at, v))
        greet((k + 1 - 2 * core, at, v))
        return carry

    lax.fori_loop(1, dom, greet_dom, 0)
    greet(twin)
    for there in (k, twin[0]):
        greet((lax.rem(there + 2, 4), j, v))
    greet((k, j, 1 - v))
    greet((lax.rem(k + 2, 4), j, 1 - v))

    load_tails = pltpu.make_async_copy(s_hbm.at[:, :, pl.ds(cols - NP, NP), :], tails, misc_sem.at[0])
    load_y = pltpu.make_async_copy(y_hbm, yop, misc_sem.at[1])
    load_speed = pltpu.make_async_copy(speed_hbm, speed, misc_sem.at[2])
    load_tails.start()
    load_y.start()
    load_speed.start()

    def load_wave(w):
        return pltpu.make_async_copy(s_hbm.at[:, w], s_own.at[w], in_sem.at[w])

    def start_wave(t, carry):
        load_wave(order(t)).start()
        return carry

    lax.fori_loop(0, waves, start_wave, 0)

    half_rows = half // 2
    own_at = pl.multiple_of(v * half, half)
    other_at = pl.multiple_of((1 - v) * half, half)
    load_g = pltpu.make_async_copy(g_hbm, gmat.at[pl.ds(own_at, half)], g_local)
    load_g.start()

    def send_g(to, queue):
        rows = pl.multiple_of(core * half_rows, half_rows)
        return remote(
            g_hbm.at[pl.ds(rows, half_rows)],
            gmat.at[pl.ds(pl.multiple_of(own_at + rows, half_rows), half_rows)],
            g_send.at[queue], g_recv.at[0], (to, j, 1 - v),
        )

    def g_twin():
        part = gmat.at[pl.ds(pl.multiple_of(other_at + core * half_rows, half_rows), half_rows)]
        return remote(part, part, g_send.at[2], g_recv.at[1], twin)

    def send_next(i, w, at):
        return remote(
            s_hbm.at[:, w, :, pl.ds(i * lanes, lanes)], s_next.at[i, w], next_send, next_recv.at[i, w], at
        )

    load_tails.wait()
    load_y.wait()
    load_speed.wait()
    yop[...] = (yop[...].astype(F32) * fine_step).astype(BF16)

    def gather_tail(w, carry):
        for p in range(2):
            rows = tails[p, w].astype(F32)
            at = pl.ds(p * waves + w, 1)
            halo_f[0, at, :] = rows[NP - 1 : NP, :]
            halo_f[1, at, :] = jnp.sum(rows * tail_ref[:, 0:1], axis=0, keepdims=True)
        return carry

    lax.fori_loop(0, waves, gather_tail, 0)
    halo_b[0] = halo_f[0].astype(BF16)
    halo_f[2] = jnp.dot(halo_b[0], yop[...], preferred_element_type=F32)

    def middle_tail(w, carry):
        keep = 1.0 - fine_step * damp_ref[w]
        cross = fine_step * coup_ref[w]
        for p in range(2):
            at = pl.ds(p * waves + w, 1)
            other = pl.ds((1 - p) * waves + w, 1)
            swap = cross if p == 0 else -cross
            halo_f[3, at, :] = (
                keep * halo_f[0, at, :]
                + halo_f[2, at, :]
                + swap * halo_f[0, other, :]
                - speed[cols - 1 : cols, :] * halo_f[1, at, :]
            )
        return carry

    lax.fori_loop(0, waves, middle_tail, 0)
    halo_b[1] = halo_f[3].astype(BF16)

    def send_halo():
        return remote(halo_b, halo_in, halo_send, halo_recv, (k, j + 1, v))

    pl.semaphore_wait(barrier, 2 * dom - 1 + 4)

    @pl.when(j < dom - 1)
    def _():
        send_halo().start()

    @pl.when(k > 0)
    def _():
        for i in range(chunks):

            def start_next(t, carry):
                send_next(i, order(t), (k - 1, j, v)).start()
                return carry

            lax.fori_loop(0, waves, start_next, 0)

    @pl.when(low)
    def _():
        send_g(k, 0).start()
        send_g(k + 2, 1).start()

    @pl.when(j > 0)
    def _():
        remote(halo_b, halo_in, halo_send, halo_recv, (k, j - 1, v)).wait_recv()
        inflow[...] = (fine_step * penalty) * halo_in[...].astype(F32)

    @pl.when(j == 0)
    def _():
        inflow[...] = jnp.zeros_like(inflow)

    first = lax.broadcasted_iota(jnp.int32, (NP, ysize), 0) == 0

    def slope_products(values):
        flat = jnp.concatenate([x.reshape(2 * cols, ysize) for x in values], axis=0)
        for at in range(0, ysize, block):
            ay[:, at : at + block] = jnp.dot(flat, yop[:, at : at + block], preferred_element_type=F32)
        for q, x in enumerate(values):
            for p in range(2):
                ax[q, p] = jnp.dot(a_ref[...], x[p], preferred_element_type=F32)

    def combine(q, w, stage, own, partner, put):
        keep = 1.0 - fine_step * damp_ref[w]
        cross = fine_step * coup_ref[w]
        for p in range(2):
            swap = cross if p == 0 else -cross
            for r in range(0, cols, NP):
                along_x = ax[q, p, r : r + NP, :]
                if r == 0:
                    row = inflow[stage, pl.ds(p * waves + w, 1), :]
                    along_x = along_x - jnp.where(first, row, 0.0)
                at = (2 * q + p) * cols + r
                put(
                    p,
                    r,
                    keep * own(p, r)
                    + ay[at : at + NP, :]
                    + swap * partner(1 - p, r)
                    - speed[r : r + NP, :] * along_x,
                )

    def emit(i, w):
        @pl.when(k < 3)
        def _():
            send_next(i, w, (k + 1, j, v)).wait_recv()
            for p in range(2):
                gap = (fine[p, w, :, i * lanes : (i + 1) * lanes] - s_next[i, w, p].astype(F32)).astype(BF16)
                target = lines.at[core, i, pl.ds(pl.multiple_of(j * cols, cols), cols)]
                mine = (w == j) & (core == p)

                @pl.when(mine)
                def _():
                    target[...] = gap

                @pl.when(jnp.logical_not(mine))
                def _():
                    dsend[i, w, p] = gap
                    remote(
                        dsend.at[i, w, p], target, line_send.at[p], line_recv.at[core, i],
                        (k - core + p, w, v),
                    ).start()

    def fine_waves(t, carry):
        ws = [order(t * pair + q) for q in range(pair)]
        for w in ws:
            load_wave(w).wait()
        slope_products([s_own[w] for w in ws])
        for q, w in enumerate(ws):

            def put_middle(p, r, value):
                mid[q, p, r : r + NP, :] = value
                midb[q, p, r : r + NP, :] = value.astype(BF16)

            def start_rows(p, r):
                return s_own[w, p, r : r + NP, :].astype(F32)

            combine(q, w, 0, start_rows, start_rows, put_middle)
        slope_products([midb[q] for q in range(pair)])
        for q, w in enumerate(ws):

            def put_fine(p, r, value):
                fine[p, w, r : r + NP, :] = value

            combine(
                q, w, 1,
                lambda p, r: mid[q, p, r : r + NP, :],
                lambda p, r: midb[q, p, r : r + NP, :].astype(F32),
                put_fine,
            )

            @pl.when(k != 1)
            def _():
                for i in range(ahead):
                    emit(i, w)

        return carry

    lax.fori_loop(0, waves // pair, fine_waves, 0)

    def emit_chunk(i):
        def step(t, carry):
            emit(i, order(t))
            return carry

        lax.fori_loop(0, waves, step, 0)

    @pl.when(k == 1)
    def _():
        for i in range(ahead):
            emit_chunk(i)

    @pl.when(k == 2)
    def _():
        for i in range(ahead, chunks):
            emit_chunk(i)

    send_g(k, 0).wait_recv()
    g_twin().start()
    load_g.wait()
    g_twin().wait_recv()

    gain = 1.0 / (1.0 + 2.0 * fine_step * jnp.full((1, lanes), damp_ref[j], F32))
    group = nz * cols

    def wait_lines(b, i, less):
        part = lines.at[b, i, pl.ds(0, (dom - less) * cols)]
        remote(part, part, line_send.at[b], line_recv.at[b, i], (k, j, v)).wait_recv()

    def spot(i, w, p):
        return c_in.at[p, w, :, pl.ds(i * lanes, lanes)]

    def send_pieces(source, i, block, to, queue):
        def step(t, carry):
            at = block * nz + lax.rem(z + t, nz)
            rows = pl.ds(pl.multiple_of(at * cols, cols), cols)
            mine = (at == j) & (k == to)

            @pl.when(mine)
            def _():
                c_in[core, j, :, i * lanes : (i + 1) * lanes] = source[rows, :]

            @pl.when(jnp.logical_not(mine))
            def _():
                remote(
                    source.at[rows], spot(i, j, core), c_send.at[queue], c_recv.at[core, i], (to, at, v)
                ).start()

            return carry

        lax.fori_loop(0, nz, step, 0)

    def product(source, out, after):
        def step(t, carry):
            block = lax.rem(y + t, ny)
            rows = pl.ds(pl.multiple_of(block * group, group), group)
            total = jnp.dot(gmat[rows, :], source[...], preferred_element_type=F32)
            out[rows, :] = (gain * total).astype(BF16)
            after(block, rows)
            return carry

        lax.fori_loop(0, ny, step, 0)

    def add_lines(target, term):
        def step(t, carry):
            rows = pl.ds(pl.multiple_of(t * cols, cols), cols)
            target[rows, :] = (target[rows, :].astype(F32) + term[rows, :].astype(F32)).astype(BF16)
            return carry

        lax.fori_loop(0, dom, step, 0)

    def across(i, block, to):
        rows = pl.ds(pl.multiple_of(block * group, group), group)
        return remote(cbuf.at[1, i, rows], lines.at[1, i, rows], x_send, x_recv.at[i * ny + block], (to, j, v))

    def give(i):
        def step(t, carry):
            send_pieces(cbuf.at[0, i], i, lax.rem(y + t, ny), 1, 0)
            return carry

        lax.fori_loop(0, ny, step, 0)

    def wait_pieces(p, i, less):
        part = cbuf.at[0, 0, pl.ds(0, (dom - less) * cols)]
        remote(part, part, c_send.at[0], c_recv.at[p, i], (k, j, v)).wait_recv()

    def wait_both(b, i):
        @pl.when(core == b)
        def _():
            wait_lines(b, i, 1)

        @pl.when(core != b)
        def _():
            wait_lines(b, i, 0)

    for i in range(chunks):
        wait_both(0, i)

        @pl.when(low)
        def _():
            product(lines.at[0, i], cbuf.at[0, i], lambda block, rows: None)

            wait_both(1, i)
            add_lines(lines.at[1, i], cbuf.at[0, i])
            product(lines.at[1, i], cbuf.at[1, i], lambda block, rows: across(i, block, k + 2).start())

            if i + ahead < chunks:
                emit_chunk(i + ahead)

            if i >= 3:
                give(i - 3)

        @pl.when(jnp.logical_not(low))
        def _():

            def forward(t, carry):
                block = lax.rem(y + t, ny)
                across(i, block, k - 2).wait_recv()
                send_pieces(lines.at[1, i], i, block, 2, 1)
                return carry

            lax.fori_loop(0, ny, forward, 0)
            add_lines(lines.at[0, i], lines.at[1, i])
            product(lines.at[0, i], cbuf.at[0, i], lambda block, rows: send_pieces(cbuf.at[0, i], i, block, 3, 0))

    @pl.when(low)
    def _():
        for i in range(chunks - 3, chunks):
            give(i)

    @pl.when(k > 0)
    def _():
        for i in range(chunks):
            for p in range(2):

                @pl.when(core == p)
                def _():
                    wait_pieces(p, i, 1)

                @pl.when(core != p)
                def _():
                    wait_pieces(p, i, 0)

            at = slice(i * lanes, (i + 1) * lanes)

            def add_change(w, carry):
                for p in range(2):
                    fine[p, w, :, at] = fine[p, w, :, at] + c_in[p, w, :, at].astype(F32)
                return carry

            lax.fori_loop(0, waves, add_change, 0)

    def done(part, send, recv):
        return remote(part, part, send, recv, (k, j, v))

    def block_of(less):
        return cbuf.at[0, :, pl.ds(0, (dom - less) * cols)]

    for p in range(2):

        @pl.when(core == p)
        def _():
            @pl.when(k < 3)
            def _():
                done(block_of(1), line_send.at[p], c_recv.at[0, 0]).wait_send()
                done(block_of(0), line_send.at[1 - p], c_recv.at[0, 0]).wait_send()

            done(block_of(p), c_send.at[0], c_recv.at[0, 0]).wait_send()

            @pl.when(jnp.logical_not(low))
            def _():
                done(block_of(1 - p), c_send.at[1], c_recv.at[0, 0]).wait_send()

    @pl.when(k > 0)
    def _():
        done(s_next, next_send, next_recv.at[0, 0]).wait_send()

    @pl.when(low)
    def _():
        done(block_of(0), x_send, c_recv.at[0, 0]).wait_send()

    @pl.when(j < dom - 1)
    def _():
        send_halo().wait_send()

    @pl.when(low)
    def _():
        send_g(k, 0).wait_send()
        send_g(k + 2, 1).wait_send()

    g_twin().wait_send()


def call(torus, state, y_operator, coarse_inverse, base_speed, damping, coupling):
    ny, nz = torus
    dom = ny * nz
    parts, waves, cols, ysize = state.shape
    assert parts == 2 and waves == dom and ysize % lanes == 0 and waves % pair == 0
    chunks = ysize // lanes
    length = dom * cols
    table = advect_matrix(cols)
    a_mat = jnp.asarray(table, BF16)
    tail = jnp.asarray(np.repeat(table[-1, -NP:, None], 128, axis=1), F32)
    anywhere = pl.BlockSpec(memory_space=pl.ANY)
    vmem = pl.BlockSpec(memory_space=pltpu.VMEM)
    smem = pl.BlockSpec(memory_space=pltpu.SMEM)
    dma = pltpu.SemaphoreType.DMA
    return pl.pallas_call(
        functools.partial(kernel, ny, nz),
        out_shape=pltpu.VMEM(state.shape, F32),
        in_specs=[anywhere] * 4 + [vmem] * 2 + [smem] * 2,
        out_specs=vmem,
        scratch_shapes=[
            pltpu.VMEM((waves, 2, cols, ysize), BF16),
            pltpu.VMEM((chunks, waves, 2, cols, lanes), BF16),
            pltpu.VMEM((2, waves, NP, ysize), BF16),
            pltpu.VMEM((ysize, ysize), BF16),
            pltpu.VMEM((cols, ysize), F32),
            pltpu.VMEM((pair, 2, cols, ysize), F32),
            pltpu.VMEM((pair, 2, cols, ysize), BF16),
            pltpu.VMEM((pair, 2, cols, ysize), F32),
            pltpu.VMEM((pair * 2 * cols, ysize), F32),
            pltpu.VMEM((4, 2 * waves, ysize), F32),
            pltpu.VMEM((2, 2 * waves, ysize), BF16),
            pltpu.VMEM((2, 2 * waves, ysize), BF16),
            pltpu.VMEM((2, 2 * waves, ysize), F32),
            pltpu.VMEM((chunks, waves, 2, cols, lanes), BF16),
            pltpu.VMEM((2, chunks, length, lanes), BF16),
            pltpu.VMEM((2, chunks, length, lanes), BF16),
            pltpu.VMEM((length, length), BF16),
            pltpu.VMEM((2, waves, cols, ysize), BF16),
            dma((waves,)),
            dma((3,)),
            dma,
            dma((chunks, waves)),
            dma((3,)),
            dma((2,)),
            dma,
            dma,
            dma,
            dma((2,)),
            dma((2, chunks)),
            dma,
            dma((chunks * ny,)),
            dma((2,)),
            dma((2, chunks)),
        ],
        compiler_params=pltpu.CompilerParams(collective_id=0, has_side_effects=True, vmem_limit_bytes=50 * 2**20),
        name="parareal",
    )(state, y_operator, coarse_inverse, base_speed, a_mat, tail, damping, coupling)


def local(torus, starts_old, y_operator, coarse_inverse, base_speed, damping, coupling):
    return call(torus, starts_old[0], y_operator, coarse_inverse, base_speed, damping, coupling)[None]


def solution(mesh):
    dom = mesh.shape["dom"]
    torus = (4, 4) if dom == 16 else (1, dom)
    in_specs = (
        P("cuts", None, "vec", "dom", None),
        P(),
        P("vec", None),
        P("dom", None),
        P("vec"),
        P("vec"),
    )
    out_specs = P("cuts", None, "vec", "dom", None)
    return jax.shard_map(
        functools.partial(local, torus), mesh=mesh, in_specs=in_specs, out_specs=out_specs, check_vma=False
    )
```

```python
import functools

import jax
import jax.numpy as jnp
import numpy as np
from jax import lax
from jax.experimental import pallas as pl
from jax.experimental.pallas import tpu as pltpu
from jax.sharding import PartitionSpec as P

NP = 16
MESH = pl.DeviceIdType.MESH
F32 = jnp.float32
BF16 = jnp.bfloat16

fine_step = 0.25
penalty = 2.0
lanes = 128
block = 256
pair = 2


def cheb_matrix(points_sub):
    indices = np.arange(points_sub)
    points = -np.cos(np.pi * indices / (points_sub - 1))
    edge_weight = np.where((indices == 0) | (indices == points_sub - 1), 2.0, 1.0)
    sign_table = np.where((indices[:, None] + indices[None, :]) % 2 == 0, 1.0, -1.0)
    identity_table = np.eye(points_sub)
    gap_matrix = points[:, None] - points[None, :] + identity_table
    off_diag = (
        edge_weight[:, None]
        / edge_weight[None, :]
        * sign_table
        / gap_matrix
        * (1.0 - identity_table)
    )
    return off_diag - off_diag.sum(axis=1)[:, None] * identity_table


def advect_matrix(columns):
    derivative = cheb_matrix(NP).astype(np.float32).astype(np.float64)
    table = np.kron(np.eye(columns // NP), derivative) * (4.0 / (NP * NP))
    for row in range(0, columns, NP):
        table[row, row] += penalty
        if row:
            table[row, row - 1] -= penalty
    return fine_step * table


def kernel(
    ny, nz, s_hbm, y_hbm, g_hbm, speed_hbm, a_ref, tail_ref, damp_ref, coup_ref,
    fine,
    s_own, s_next, tails, yop, speed, mid, midb, ax, ay, halo_f, halo_b, halo_in, inflow,
    dsend, lines, cbuf, gmat, c_in,
    in_sem, misc_sem, next_send, next_recv, g_send, g_recv, g_local, halo_send, halo_recv,
    line_send, line_recv, x_send, x_recv, c_send, c_recv,
):
    k = lax.axis_index("cuts")
    j = lax.axis_index("dom")
    v = lax.axis_index("vec")
    y, z = j // nz, lax.rem(j, nz)
    core = lax.rem(k, 2)
    low = k < 2
    dom = ny * nz
    _, waves, cols, ysize = s_hbm.shape
    chunks = ysize // lanes
    half = g_hbm.shape[0]
    ahead = chunks // 2
    quarter = half // 4

    def order(t):
        ty = lax.rem(t, ny)
        tz = lax.rem(t // ny + (nz - 1) * ty, nz)
        return lax.rem(y + ty, ny) * nz + lax.rem(z + tz, nz)

    def remote(src, dst, send, recv, at):
        return pltpu.make_async_remote_copy(
            src_ref=src, dst_ref=dst, send_sem=send, recv_sem=recv, device_id=at, device_id_type=MESH
        )

    twin = (k + 1 - 2 * core, j, v)
    barrier = pltpu.get_barrier_semaphore()

    def greet(at):
        pl.semaphore_signal(barrier, inc=1, device_id=at, device_id_type=MESH)

    def greet_dom(t, carry):
        at = lax.rem(j + t, dom)
        greet((k, at, v))
        greet((k + 1 - 2 * core, at, v))
        return carry

    lax.fori_loop(1, dom, greet_dom, 0)
    greet(twin)
    for there in (k, twin[0]):
        greet((lax.rem(there + 2, 4), j, v))
    greet((k, j, 1 - v))
    greet((lax.rem(k + 2, 4), j, 1 - v))

    load_tails = pltpu.make_async_copy(s_hbm.at[:, :, pl.ds(cols - NP, NP), :], tails, misc_sem.at[0])
    load_y = pltpu.make_async_copy(y_hbm, yop, misc_sem.at[1])
    load_speed = pltpu.make_async_copy(speed_hbm, speed, misc_sem.at[2])
    load_tails.start()
    load_y.start()
    load_speed.start()

    def load_wave(w):
        return pltpu.make_async_copy(s_hbm.at[:, w], s_own.at[w], in_sem.at[w])

    def start_wave(t, carry):
        load_wave(order(t)).start()
        return carry

    lax.fori_loop(0, waves, start_wave, 0)

    half_rows = half // 2
    own_at = pl.multiple_of(v * half, half)
    other_at = pl.multiple_of((1 - v) * half, half)
    load_g = pltpu.make_async_copy(g_hbm, gmat.at[pl.ds(own_at, half)], g_local)
    load_g.start()

    def send_g(to, queue):
        rows = pl.multiple_of(core * half_rows, half_rows)
        return remote(
            g_hbm.at[pl.ds(rows, half_rows)],
            gmat.at[pl.ds(pl.multiple_of(own_at + rows, half_rows), half_rows)],
            g_send.at[queue], g_recv.at[0], (to, j, 1 - v),
        )

    def g_twin():
        part = gmat.at[pl.ds(pl.multiple_of(other_at + core * half_rows, half_rows), half_rows)]
        return remote(part, part, g_send.at[2], g_recv.at[1], twin)

    def send_next(i, w, at):
        return remote(
            s_hbm.at[:, w, :, pl.ds(i * lanes, lanes)], s_next.at[i, w], next_send, next_recv.at[i, w], at
        )

    pl.semaphore_wait(barrier, 2 * dom - 1 + 4)

    @pl.when(k > 0)
    def _():
        for i in range(chunks):

            def start_next(t, carry):
                send_next(i, order(t), (k - 1, j, v)).start()
                return carry

            lax.fori_loop(0, waves, start_next, 0)

    @pl.when(low)
    def _():
        send_g(k, 0).start()
        send_g(k + 2, 1).start()

    load_tails.wait()
    load_y.wait()
    load_speed.wait()
    yop[...] = (yop[...].astype(F32) * fine_step).astype(BF16)

    def gather_tail(w, carry):
        for p in range(2):
            rows = tails[p, w].astype(F32)
            at = pl.ds(p * waves + w, 1)
            halo_f[0, at, :] = rows[NP - 1 : NP, :]
            halo_f[1, at, :] = jnp.sum(rows * tail_ref[:, 0:1], axis=0, keepdims=True)
        return carry

    lax.fori_loop(0, waves, gather_tail, 0)
    halo_b[0] = halo_f[0].astype(BF16)
    halo_f[2] = jnp.dot(halo_b[0], yop[...], preferred_element_type=F32)

    def middle_tail(w, carry):
        keep = 1.0 - fine_step * damp_ref[w]
        cross = fine_step * coup_ref[w]
        for p in range(2):
            at = pl.ds(p * waves + w, 1)
            other = pl.ds((1 - p) * waves + w, 1)
            swap = cross if p == 0 else -cross
            halo_f[3, at, :] = (
                keep * halo_f[0, at, :]
                + halo_f[2, at, :]
                + swap * halo_f[0, other, :]
                - speed[cols - 1 : cols, :] * halo_f[1, at, :]
            )
        return carry

    lax.fori_loop(0, waves, middle_tail, 0)
    halo_b[1] = halo_f[3].astype(BF16)

    def send_halo():
        return remote(halo_b, halo_in, halo_send, halo_recv, (k, j + 1, v))

    @pl.when(j < dom - 1)
    def _():
        send_halo().start()

    @pl.when(j > 0)
    def _():
        remote(halo_b, halo_in, halo_send, halo_recv, (k, j - 1, v)).wait_recv()
        inflow[...] = (fine_step * penalty) * halo_in[...].astype(F32)

    @pl.when(j == 0)
    def _():
        inflow[...] = jnp.zeros_like(inflow)

    first = lax.broadcasted_iota(jnp.int32, (NP, ysize), 0) == 0

    def slope_products(values):
        flat = jnp.concatenate([x.reshape(2 * cols, ysize) for x in values], axis=0)
        for at in range(0, ysize, block):
            ay[:, at : at + block] = jnp.dot(flat, yop[:, at : at + block], preferred_element_type=F32)
        for q, x in enumerate(values):
            for p in range(2):
                ax[q, p] = jnp.dot(a_ref[...], x[p], preferred_element_type=F32)

    def combine(q, w, stage, own, partner, put):
        keep = 1.0 - fine_step * damp_ref[w]
        cross = fine_step * coup_ref[w]
        for p in range(2):
            swap = cross if p == 0 else -cross
            for r in range(0, cols, NP):
                along_x = ax[q, p, r : r + NP, :]
                if r == 0:
                    row = inflow[stage, pl.ds(p * waves + w, 1), :]
                    along_x = along_x - jnp.where(first, row, 0.0)
                at = (2 * q + p) * cols + r
                put(
                    p,
                    r,
                    keep * own(p, r)
                    + ay[at : at + NP, :]
                    + swap * partner(1 - p, r)
                    - speed[r : r + NP, :] * along_x,
                )

    def emit(i, w):
        @pl.when(k < 3)
        def _():
            send_next(i, w, (k + 1, j, v)).wait_recv()
            for p in range(2):
                gap = (fine[p, w, :, i * lanes : (i + 1) * lanes] - s_next[i, w, p].astype(F32)).astype(BF16)
                target = lines.at[core, i, pl.ds(pl.multiple_of(j * cols, cols), cols)]
                mine = (w == j) & (core == p)

                @pl.when(mine)
                def _():
                    target[...] = gap

                @pl.when(jnp.logical_not(mine))
                def _():
                    dsend[i, w, p] = gap
                    remote(
                        dsend.at[i, w, p], target, line_send.at[p], line_recv.at[core, i],
                        (k - core + p, w, v),
                    ).start()

    def fine_waves(t, carry):
        ws = [order(t * pair + q) for q in range(pair)]
        for w in ws:
            load_wave(w).wait()
        slope_products([s_own[w] for w in ws])
        for q, w in enumerate(ws):

            def put_middle(p, r, value):
                mid[q, p, r : r + NP, :] = value
                midb[q, p, r : r + NP, :] = value.astype(BF16)

            def start_rows(p, r):
                return s_own[w, p, r : r + NP, :].astype(F32)

            combine(q, w, 0, start_rows, start_rows, put_middle)
        slope_products([midb[q] for q in range(pair)])
        for q, w in enumerate(ws):

            def put_fine(p, r, value):
                fine[p, w, r : r + NP, :] = value

            combine(
                q, w, 1,
                lambda p, r: mid[q, p, r : r + NP, :],
                lambda p, r: midb[q, p, r : r + NP, :].astype(F32),
                put_fine,
            )

            @pl.when(k != 1)
            def _():
                for i in range(ahead):
                    emit(i, w)

        return carry

    lax.fori_loop(0, waves // pair, fine_waves, 0)

    def emit_chunk(i):
        def step(t, carry):
            emit(i, order(t))
            return carry

        lax.fori_loop(0, waves, step, 0)

    @pl.when(k == 1)
    def _():
        for i in range(ahead):
            emit_chunk(i)

    @pl.when(k == 2)
    def _():
        for i in range(ahead, chunks):
            emit_chunk(i)

    send_g(k, 0).wait_recv()
    g_twin().start()
    load_g.wait()
    g_twin().wait_recv()

    gain = 1.0 / (1.0 + 2.0 * fine_step * jnp.full((1, lanes), damp_ref[j], F32))
    group = nz * cols

    def wait_lines(b, i, less):
        part = lines.at[b, i, pl.ds(0, (dom - less) * cols)]
        remote(part, part, line_send.at[b], line_recv.at[b, i], (k, j, v)).wait_recv()

    def spot(i, w, p):
        return c_in.at[p, w, :, pl.ds(i * lanes, lanes)]

    def send_pieces(source, i, block, to, queue):
        def step(t, carry):
            at = block * nz + lax.rem(z + t, nz)
            rows = pl.ds(pl.multiple_of(at * cols, cols), cols)
            mine = (at == j) & (k == to)

            @pl.when(mine)
            def _():
                c_in[core, j, :, i * lanes : (i + 1) * lanes] = source[rows, :]

            @pl.when(jnp.logical_not(mine))
            def _():
                remote(
                    source.at[rows], spot(i, j, core), c_send.at[queue], c_recv.at[core, i], (to, at, v)
                ).start()

            return carry

        lax.fori_loop(0, nz, step, 0)

    def product(source, out, after):
        def step(t, carry):
            block = lax.rem(y + t, ny)
            rows = pl.ds(pl.multiple_of(block * group, group), group)
            total = jnp.dot(gmat[rows, :], source[...], preferred_element_type=F32)
            out[rows, :] = (gain * total).astype(BF16)
            after(block, rows)
            return carry

        lax.fori_loop(0, ny, step, 0)

    def add_lines(target, term):
        def step(t, carry):
            rows = pl.ds(pl.multiple_of(t * cols, cols), cols)
            target[rows, :] = (target[rows, :].astype(F32) + term[rows, :].astype(F32)).astype(BF16)
            return carry

        lax.fori_loop(0, dom, step, 0)

    def across(i, block, to):
        rows = pl.ds(pl.multiple_of(block * group, group), group)
        return remote(cbuf.at[1, i, rows], lines.at[1, i, rows], x_send, x_recv.at[i * ny + block], (to, j, v))

    def give(i):
        def step(t, carry):
            send_pieces(cbuf.at[0, i], i, lax.rem(y + t, ny), 1, 0)
            return carry

        lax.fori_loop(0, ny, step, 0)

    def wait_pieces(p, i, less):
        part = cbuf.at[0, 0, pl.ds(0, (dom - less) * cols)]
        remote(part, part, c_send.at[0], c_recv.at[p, i], (k, j, v)).wait_recv()

    def wait_both(b, i):
        @pl.when(core == b)
        def _():
            wait_lines(b, i, 1)

        @pl.when(core != b)
        def _():
            wait_lines(b, i, 0)

    for i in range(chunks):
        wait_both(0, i)

        @pl.when(low)
        def _():
            product(lines.at[0, i], cbuf.at[0, i], lambda block, rows: None)

            wait_both(1, i)
            add_lines(lines.at[1, i], cbuf.at[0, i])
            product(lines.at[1, i], cbuf.at[1, i], lambda block, rows: across(i, block, k + 2).start())

            if i + ahead < chunks:
                emit_chunk(i + ahead)

            if i >= 3:
                give(i - 3)

        @pl.when(jnp.logical_not(low))
        def _():

            def forward(t, carry):
                block = lax.rem(y + t, ny)
                across(i, block, k - 2).wait_recv()
                send_pieces(lines.at[1, i], i, block, 2, 1)
                return carry

            lax.fori_loop(0, ny, forward, 0)
            add_lines(lines.at[0, i], lines.at[1, i])
            product(lines.at[0, i], cbuf.at[0, i], lambda block, rows: send_pieces(cbuf.at[0, i], i, block, 3, 0))

    @pl.when(low)
    def _():
        for i in range(chunks - 3, chunks):
            give(i)

    @pl.when(k > 0)
    def _():
        for i in range(chunks):
            for p in range(2):

                @pl.when(core == p)
                def _():
                    wait_pieces(p, i, 1)

                @pl.when(core != p)
                def _():
                    wait_pieces(p, i, 0)

            at = slice(i * lanes, (i + 1) * lanes)

            def add_change(w, carry):
                for p in range(2):
                    fine[p, w, :, at] = fine[p, w, :, at] + c_in[p, w, :, at].astype(F32)
                return carry

            lax.fori_loop(0, waves, add_change, 0)

    def done(part, send, recv):
        return remote(part, part, send, recv, (k, j, v))

    def block_of(less):
        return cbuf.at[0, :, pl.ds(0, (dom - less) * cols)]

    for p in range(2):

        @pl.when(core == p)
        def _():
            @pl.when(k < 3)
            def _():
                done(block_of(1), line_send.at[p], c_recv.at[0, 0]).wait_send()
                done(block_of(0), line_send.at[1 - p], c_recv.at[0, 0]).wait_send()

            done(block_of(p), c_send.at[0], c_recv.at[0, 0]).wait_send()

            @pl.when(jnp.logical_not(low))
            def _():
                done(block_of(1 - p), c_send.at[1], c_recv.at[0, 0]).wait_send()

    @pl.when(k > 0)
    def _():
        done(s_next, next_send, next_recv.at[0, 0]).wait_send()

    @pl.when(low)
    def _():
        done(block_of(0), x_send, c_recv.at[0, 0]).wait_send()

    @pl.when(j < dom - 1)
    def _():
        send_halo().wait_send()

    @pl.when(low)
    def _():
        send_g(k, 0).wait_send()
        send_g(k + 2, 1).wait_send()

    g_twin().wait_send()


def call(torus, state, y_operator, coarse_inverse, base_speed, damping, coupling):
    ny, nz = torus
    dom = ny * nz
    parts, waves, cols, ysize = state.shape
    assert parts == 2 and waves == dom and ysize % lanes == 0 and waves % pair == 0
    chunks = ysize // lanes
    length = dom * cols
    table = advect_matrix(cols)
    a_mat = jnp.asarray(table, BF16)
    tail = jnp.asarray(np.repeat(table[-1, -NP:, None], 128, axis=1), F32)
    anywhere = pl.BlockSpec(memory_space=pl.ANY)
    vmem = pl.BlockSpec(memory_space=pltpu.VMEM)
    smem = pl.BlockSpec(memory_space=pltpu.SMEM)
    dma = pltpu.SemaphoreType.DMA
    return pl.pallas_call(
        functools.partial(kernel, ny, nz),
        out_shape=pltpu.VMEM(state.shape, F32),
        in_specs=[anywhere] * 4 + [vmem] * 2 + [smem] * 2,
        out_specs=vmem,
        scratch_shapes=[
            pltpu.VMEM((waves, 2, cols, ysize), BF16),
            pltpu.VMEM((chunks, waves, 2, cols, lanes), BF16),
            pltpu.VMEM((2, waves, NP, ysize), BF16),
            pltpu.VMEM((ysize, ysize), BF16),
            pltpu.VMEM((cols, ysize), F32),
            pltpu.VMEM((pair, 2, cols, ysize), F32),
            pltpu.VMEM((pair, 2, cols, ysize), BF16),
            pltpu.VMEM((pair, 2, cols, ysize), F32),
            pltpu.VMEM((pair * 2 * cols, ysize), F32),
            pltpu.VMEM((4, 2 * waves, ysize), F32),
            pltpu.VMEM((2, 2 * waves, ysize), BF16),
            pltpu.VMEM((2, 2 * waves, ysize), BF16),
            pltpu.VMEM((2, 2 * waves, ysize), F32),
            pltpu.VMEM((chunks, waves, 2, cols, lanes), BF16),
            pltpu.VMEM((2, chunks, length, lanes), BF16),
            pltpu.VMEM((2, chunks, length, lanes), BF16),
            pltpu.VMEM((length, length), BF16),
            pltpu.VMEM((2, waves, cols, ysize), BF16),
            dma((waves,)),
            dma((3,)),
            dma,
            dma((chunks, waves)),
            dma((3,)),
            dma((2,)),
            dma,
            dma,
            dma,
            dma((2,)),
            dma((2, chunks)),
            dma,
            dma((chunks * ny,)),
            dma((2,)),
            dma((2, chunks)),
        ],
        compiler_params=pltpu.CompilerParams(collective_id=0, has_side_effects=True, vmem_limit_bytes=50 * 2**20),
        name="parareal",
    )(state, y_operator, coarse_inverse, base_speed, a_mat, tail, damping, coupling)


def local(torus, starts_old, y_operator, coarse_inverse, base_speed, damping, coupling):
    return call(torus, starts_old[0], y_operator, coarse_inverse, base_speed, damping, coupling)[None]


def solution(mesh):
    dom = mesh.shape["dom"]
    torus = (4, 4) if dom == 16 else (1, dom)
    in_specs = (
        P("cuts", None, "vec", "dom", None),
        P(),
        P("vec", None),
        P("dom", None),
        P("vec"),
        P("vec"),
    )
    out_specs = P("cuts", None, "vec", "dom", None)
    return jax.shard_map(
        functools.partial(local, torus), mesh=mesh, in_specs=in_specs, out_specs=out_specs, check_vma=False
    )
```
